128 devices in a mesh: row: 8 (over y, core), col: 16 (over x, z).
Axes of the slice: x: 4, y: 4, z: 4, core: 2. Of those that a mesh axis runs over, the one named last changes fastest.
Arguments:
- upper_a: bfloat16 [2, 4096, 8192], P(None, 'row', 'col'), may hold values from -0.125 to 0.125
- upper_b: bfloat16 [4, 4096, 2, 8192], P(None, 'row', None, 'col'), may hold values from -0.125 to 0.125
- right_side: bfloat16 [2, 4096, 2, 8192], P(None, 'row', None, 'col'), may hold values from -6 to 6
- a_bases: bfloat16 [2, 4096, 512], P(None, 'row'), may hold values from -1 to 1, as said below
- b_bases: bfloat16 [2, 8192, 512], P(None, 'col'), may hold values from -1 to 1, as said below
- a_values: float32 [2, 4096], P(None, 'row'), may hold values from 0.25 to 4
- b_values: float32 [2, 8192], P(None, 'col'), may hold values from 0.25 to 4
Outputs:
- solution: float32 [2, 4096, 2, 8192], P(None, 'row', None, 'col')
The draws below stay inside these ranges and needn't reach their ends.
Inputs may be any that keep to these rules, and one draw needn't show every extreme that they name: Each tile of a_bases is an orthonormal matrix rounded to bfloat16. Each tile of b_bases is an orthonormal matrix rounded to bfloat16.
All inputs are finite; a program needn't handle non-finite values.
Results may differ from the reference program's by a relative error of at most 0.012.
Values may be sent and summed in bfloat16 or wider, within the bound.
A program may use at most 128 MiB of HBM per device.

```python
import math
import jax
import jax.numpy as jnp
from jax import lax

NB = 512
CT = 2
FRONTS = 4
TR = 16
RT = 2
TC = 32
BR = 4
M = 8192
FIRST = 14
N_ROW = 8
N_COL = 16


def orthonormal(key, tile_count):
    samples = jax.random.normal(key, (tile_count, NB, NB), jnp.float32)
    factor, triangle = jnp.linalg.qr(samples)
    return factor


def draw_a_bases(key, part):
    return orthonormal(jax.random.fold_in(key, 11), TR).reshape(RT, N_ROW * NB, NB).astype(jnp.bfloat16)


def draw_b_bases(key, part):
    return orthonormal(jax.random.fold_in(key, 23), TC).reshape(CT, N_COL * NB, NB).astype(jnp.bfloat16)


def level_of(stream_key, dims, pieces, low, largest):
    level = 1.0
    for dim, blocks in pieces:
        draws = jax.random.uniform(jax.random.fold_in(jax.random.fold_in(stream_key, 6), dim), (blocks,), jnp.float32, low / len(pieces), largest / len(pieces))
        level = level * jnp.repeat(jnp.exp(draws), dims[dim] // blocks).reshape((-1,) + (1,) * (len(dims) - 1 - dim))
    return level


def normal_values(own_key, extent, spread, limit, pieces=(), kind=jnp.bfloat16):
    result = spread * jax.random.normal(own_key, extent, jnp.float32)
    if pieces:
        result = result * level_of(own_key, extent, pieces, -0.22, 0.18)
    return jnp.clip(result, -limit, limit).astype(kind)


def setup_inputs(seed: int = 0) -> dict:
    streams_of = jax.random.split(jax.random.key(seed), 8)
    return {
        "upper_a": normal_values(streams_of[0], (RT, N_ROW * NB, M), (4 * NB) ** -0.5, 0.125, ((1, 8), (2, 16))),
        "upper_b": normal_values(streams_of[1], (BR, N_ROW * NB, CT, N_COL * NB), (4 * NB) ** -0.5, 0.125, ((1, 8), (3, 16))),
        "right_side": normal_values(streams_of[2], (RT, N_ROW * NB, CT, N_COL * NB), 1.0, 6.0, ((1, 8), (3, 16))),
        "a_bases": draw_a_bases(jax.random.fold_in(streams_of[7], 71), 0),
        "b_bases": draw_b_bases(jax.random.fold_in(streams_of[7], 71), 0),
        "a_values": jnp.clip(jnp.exp(math.log(4.0) - 2.7725887 * jax.random.uniform(streams_of[5], (RT, N_ROW * NB), jnp.float32) ** level_of(streams_of[5], (RT, N_ROW * NB), ((1, 8),), -0.2, 0.2)), 0.25, 4.0),
        "b_values": jnp.clip(jnp.exp(math.log(4.0) - 2.7725887 * jax.random.uniform(streams_of[6], (CT, N_COL * NB), jnp.float32) ** level_of(streams_of[6], (CT, N_COL * NB), ((1, 16),), -0.2, 0.2)), 0.25, 4.0),
    }


def rounded_copy(value):
    return lax.optimization_barrier(value.astype(jnp.bfloat16)).astype(jnp.float32)

def solve_tiles(waiting, basis_left, values_left, basis_right, values_right):
    highest = lax.Precision.HIGHEST
    left_full = basis_left.astype(jnp.float32)
    right_full = basis_right.astype(jnp.float32)
    rounded = rounded_copy(waiting)
    first_half = rounded_copy(jnp.einsum('npq,npr->nqr', left_full, rounded, precision=highest))
    scaled = jnp.einsum('nqr,nrs->nqs', first_half, right_full, precision=highest)
    scaled = rounded_copy(scaled / (values_left[:, :, None] + values_right[:, None, :]))
    left_side = rounded_copy(jnp.einsum('npq,nqs->nps', left_full, scaled, precision=highest))
    return jnp.einsum('nps,nts->npt', left_side, right_full, precision=highest).astype(jnp.bfloat16)

def reference(upper_a, upper_b, right_side, a_bases, b_bases, a_values, b_values):
    highest = lax.Precision.HIGHEST
    working = right_side.astype(jnp.float32).reshape(TR, NB, TC, NB)
    matrix_a = upper_a.astype(jnp.float32).reshape(TR, NB, TR, NB)
    matrix_b = upper_b.astype(jnp.float32).reshape(TC, NB, TC, NB)
    bases_left = a_bases.reshape(TR, NB, NB)
    bases_right = b_bases.reshape(TC, NB, NB)
    values_left = a_values.reshape(TR, NB)
    values_right = b_values.reshape(TC, NB)
    tile_i = jnp.arange(TR, dtype=jnp.int32)
    tile_j = jnp.arange(TC, dtype=jnp.int32)
    for front_step in range(FRONTS):
        front_id = FIRST + front_step
        k_glob = TR - 1 - front_id + tile_j
        k_valid = (k_glob >= 0) & (k_glob <= TR - 1)
        k_safe = jnp.clip(k_glob, 0, TR - 1)
        waiting = working[k_safe, :, tile_j, :]
        solved = solve_tiles(waiting, bases_left[k_safe], values_left[k_safe], bases_right, values_right)
        solved = jnp.where(k_valid[:, None, None], solved, jnp.zeros_like(solved))
        solved_full = solved.astype(jnp.float32)
        working = working.at[k_safe, :, tile_j, :].set(jnp.where(k_valid[:, None, None], solved_full, waiting))
        column_terms = jnp.einsum('ipjq,jqr->ipjr', matrix_a[:, :, k_safe, :], solved_full, precision=highest)
        column_mask = (k_valid[None, :] & (tile_i[:, None] < k_glob[None, :])).astype(jnp.float32)
        l_glob = front_id - TR + 1 + tile_i
        l_safe = jnp.clip(l_glob, 0, TC - 1)
        row_terms = jnp.einsum('ipq,iqjr->ipjr', solved_full[l_safe], matrix_b[l_safe], precision=highest)
        row_mask = ((l_glob[:, None] >= 0) & (l_glob[:, None] < tile_j[None, :])).astype(jnp.float32)
        working = working - column_terms * column_mask[:, None, :, None] - row_terms * row_mask[:, None, :, None]
    return working.reshape(RT, N_ROW * NB, CT, N_COL * NB)
```

```python
import functools

import jax
import jax.numpy as jnp
from jax import lax
from jax.experimental import pallas as pl
from jax.experimental.pallas import tpu as pltpu
from jax.sharding import PartitionSpec as P

MESH = pl.DeviceIdType.MESH
FRONTS = 4
RING = 4
PIECES = 2


def plan(nb, n_row, n_col, a_in, b_in, c_in, qa_in, qb_in, av_in, bv_in, out,
         a_buf, b_buf, xc, xr, w, c_buf, qa, qat, qb, inv, half, av, bv,
         local_sem, out_sem, a_send, b_send, a_recv, b_recv, xc_send, xr_send, xc_recv, xr_recv):
    rows = nb // PIECES
    r = lax.axis_index("row")
    c = lax.axis_index("col")
    y, core = r // 2, r % 2
    x, z = c // RING, c % RING
    mod = lax.rem

    def row_of(yy, kk):
        return mod(yy + 2 * RING, RING) * 2 + kk

    def col_of(xx, zz):
        return mod(xx + 2 * RING, RING) * RING + mod(zz + 2 * RING, RING)

    col_next = mod(c + 1, n_col)
    col_prev = mod(c + n_col - 1, n_col)

    shift = mod(c - r + 1 + n_col, n_col)
    turn = mod(shift, 8)
    a_own = shift // 8
    l_own = r + 8 * a_own - 1 + turn
    b_own = jnp.where(l_own >= n_col, 1, 0)
    solves = (turn < FRONTS) & (l_own >= 0)
    turn = jnp.where(solves, turn, 99)

    def remote(src, dst, send, recv, row, col):
        return pltpu.make_async_remote_copy(
            src_ref=src, dst_ref=dst, send_sem=send, recv_sem=recv,
            device_id=(row, col), device_id_type=MESH)

    def k_of(s, col):
        return mod(col + 1 - s + n_col, n_col)

    def has_col(s, col):
        return jnp.logical_not((s == 0) & (col == n_col - 1))

    def needs_a(s, row, col, a):
        return has_col(s, col) & (row + 8 * a < k_of(s, col))

    def needs_b(s, row, col, a, b):
        l = row + 8 * a - 1 + s
        return (l >= 0) & (l < col + n_col * b)

    def a_copy(s, a, col, src):
        return remote(src, a_buf.at[s, a], a_send.at[s, a], a_recv.at[s, a], r, col)

    def b_copy(s, a, b, row, src):
        return remote(src, b_buf.at[s, a, b], b_send.at[s, a, b], b_recv.at[s, a, b], row, c)

    def hand_b(a, b):
        return remote(b_buf.at[2, a, b], b_buf.at[3, a, b], b_send.at[1, a, b], b_recv.at[3, a, b], partner, c)

    def each_a(fn):
        for a in range(2):
            fn(a)

    def each_ab(fn):
        for a in range(2):
            for b in range(2):
                fn(a, b)

    def send_a(s, col):
        def one(a):
            @pl.when(needs_a(s, r, col, a))
            def _():
                a_copy(s, a, col, a_in.at[a]).start()
        each_a(one)

    def send_b(s, row):
        def one(a, b):
            @pl.when(needs_b(s, row, c, a, b))
            def _():
                l4 = (row + 8 * a - 1 + s) // 8
                b_copy(s, a, b, row, b_in.at[l4, b]).start()
        each_ab(one)

    row_next = mod(r + 1, n_row)
    row_prev = mod(r + n_row - 1, n_row)
    row_prev2 = mod(r + n_row - 2, n_row)
    partner = y * 2 + 1 - core

    def col_route(s, q):
        g = 1 if q % 2 == 0 else -1
        k = k_of(s, c)
        rr = mod(k, 8)
        ry = rr // 2
        valid = has_col(s, c)
        root = valid & (r == rr)
        oy = mod((y - ry) * g + RING, RING)
        relay = valid & (oy != 0) & (core == 1)
        piece = pl.ds(q * rows, rows)

        def copy(n, row):
            return remote(xc.at[s, piece], xc.at[s, piece], xc_send.at[s, q, n], xc_recv.at[s, q], row, c)

        sends = [
            (root | (relay & (oy == 1)), copy(0, row_of(y + g, 1))),
            (root, copy(1, row_of(y - g, 1))),
            (root | relay, copy(2, partner)),
        ]
        return valid & (r != rr), sends, copy(2, partner)

    def row_route(s, a, q):
        g = 1 if q % 2 == 0 else -1
        l = r + 8 * a - 1 + s
        valid = l >= 0
        lc = mod(l + n_col, n_col)
        rx, rz = lc // RING, lc % RING
        root = valid & (c == lc)
        oz = mod((z - rz) * g + RING, RING)
        ox = mod((x - rx) * g + RING, RING)
        early = (rz == RING - 1) & (z == 0) & (ox == 0)
        forth = valid & ((ox == 0) | (ox == 1))
        back = valid & (ox == 0)
        if g == 1:
            forth = forth & jnp.logical_not(early)
        else:
            back = back & jnp.logical_not(early)
        piece = pl.ds(q * rows, rows)

        def copy(n, col):
            return remote(xr.at[s, a, piece], xr.at[s, a, piece], xr_send.at[s, a, q, n], xr_recv.at[s, a, q], r, col)

        sends = [
            (valid & (ox == 0) & ((oz == 0) | (oz == 1)), copy(0, col_of(x, z + g))),
            (root & (rz == RING - 1), copy(4, col_next)),
            (valid & (ox == 0) & (oz == 0), copy(1, col_of(x, z - g))),
            (forth, copy(2, col_of(x + g, z))),
            (back, copy(3, col_of(x - g, z))),
        ]
        return valid & (c != lc), sends, copy(0, col_of(x, z + g))

    def launch(sends):
        for when, copy in sends:
            @pl.when(when)
            def _(copy=copy):
                copy.start()

    def collect(sends):
        for when, copy in sends:
            @pl.when(when)
            def _(copy=copy):
                copy.wait_send()

    def take_col(s):
        for q in range(PIECES):
            arrives, sends, copy = col_route(s, q)

            @pl.when(arrives)
            def _():
                copy.wait_recv()
                launch(sends)

    def take_row(s, a):
        for q in range(PIECES):
            arrives, sends, copy = row_route(s, a, q)

            @pl.when(arrives)
            def _():
                copy.wait_recv()
                launch(sends)

    f32 = jnp.float32

    def matmul(p, q):
        return jnp.dot(p, q, preferred_element_type=f32)

    def update(s, a, b):
        i, j = r + 8 * a, c + n_col * b
        k = j + 1 - s

        @pl.when((k >= 0) & (k < n_col) & (i < k))
        def _():
            @pl.when(s != 2)
            def _():
                a_copy(s, a, c, a_buf.at[s, a]).wait_recv()
            w[a, b] = w[a, b] - matmul(a_buf[s, a], xc[s])

        @pl.when(needs_b(s, r, c, a, b))
        def _():
            @pl.when(s != 2)
            def _():
                b_copy(s, a, b, r, b_buf.at[s, a, b]).wait_recv()
            w[a, b] = w[a, b] - matmul(xr[s, a], b_buf[s, a, b])

    def solve(s):
        half[0] = w[a_own, b_own].astype(jnp.bfloat16)
        half[1] = matmul(qat[...], half[0]).astype(jnp.bfloat16)
        half[0] = (matmul(half[1], qb[...]) * inv[...]).astype(jnp.bfloat16)
        for q in range(PIECES):
            piece = pl.ds(q * rows, rows)
            left = matmul(qa[piece, :], half[0]).astype(jnp.bfloat16)
            tile = lax.dot_general(left, qb[...], (((1,), (1,)), ((), ())), preferred_element_type=f32)
            tile = tile.astype(jnp.bfloat16)
            xr[s, a_own, piece, :] = tile
            xc[s, piece, :] = tile
            w[a_own, b_own, piece, :] = tile.astype(f32)
            _, sends, _ = col_route(s, q)
            launch(sends)
            _, sends, _ = row_route(s, a_own, q)
            launch(sends)

    barrier = pltpu.get_barrier_semaphore()
    friends = [(partner, c), (r, col_next), (r, col_prev)]
    for d in (1, -1):
        friends += [(row_of(y + d, 0), c), (row_of(y + d, 1), c), (r, col_of(x, z + d)), (r, col_of(x + d, z))]
    for friend in friends:
        pl.semaphore_signal(barrier, inc=1, device_id=friend, device_id_type=MESH)

    loads = [
        pltpu.make_async_copy(c_in, c_buf, local_sem.at[0]),
        pltpu.make_async_copy(qa_in.at[a_own], qa, local_sem.at[1]),
        pltpu.make_async_copy(qb_in.at[b_own], qb, local_sem.at[2]),
        pltpu.make_async_copy(av_in.at[a_own], av, local_sem.at[3]),
        pltpu.make_async_copy(bv_in.at[b_own], bv, local_sem.at[4]),
    ]
    for load in loads:
        load.start()

    def local_a(a):
        return pltpu.make_async_copy(a_in.at[a], a_buf.at[1, a], a_recv.at[1, a])

    def local_b(a, b):
        return pltpu.make_async_copy(b_in.at[a, b], b_buf.at[1, a, b], b_recv.at[1, a, b])

    each_a(lambda a: pl.when(needs_a(1, r, c, a))(lambda: local_a(a).start()))
    each_ab(lambda a, b: pl.when(needs_b(1, r, c, a, b))(lambda: local_b(a, b).start()))

    pl.semaphore_wait(barrier, len(friends))
    send_a(0, col_prev)
    send_b(0, row_next)

    for load in loads:
        load.wait()

    @pl.when(solves)
    def _():
        qat[...] = qa[...].T
        down = jnp.broadcast_to(av[...], (128, nb)).T
        for n in range(nb // 128):
            lanes = pl.ds(n * 128, 128)
            inv[:, lanes] = 1.0 / (down + bv[:, lanes])

    def load_w(t, carry):
        w[t // 2, t % 2] = c_buf[t // 2, t % 2].astype(f32)
        return carry
    lax.fori_loop(0, 4, load_w, 0)

    def front(t, carry):
        s = t - 1

        @pl.when(t > 0)
        def _():
            take_col(s)
            take_row(s, jnp.where(solves, a_own, a_near(s)))

        ahead = turn == t

        @pl.when(ahead)
        def _():
            @pl.when(t > 0)
            def _():
                update(s, a_own, b_own)
            solve(t)

        @pl.when(t == 1)
        def _():
            send_a(2, col_next)
            send_b(2, row_prev)

        @pl.when(t > 0)
        def _():
            take_row(s, 1 - jnp.where(solves, a_own, a_near(s)))

            def rest(n, carry):
                a, b = n // 2, n % 2

                @pl.when(jnp.logical_not(ahead & (a == a_own) & (b == b_own)))
                def _():
                    update(s, a, b)

                @pl.when(t == FRONTS)
                def _():
                    pltpu.make_async_copy(w.at[a, b], out.at[a, b], out_sem.at[a, b]).start()
                return carry
            lax.fori_loop(0, 4, rest, 0)

        @pl.when(t == 2)
        def _():
            relay_two()
        return carry

    def a_near(s):
        l = mod(r - 1 + s + n_col, n_col)
        gap = mod(x - l // RING + RING, RING)
        return jnp.where((gap == 0) | (gap == 1), 0, 1)

    def relay_two():
        def one(a):
            @pl.when(needs_a(2, r, c, a))
            def _():
                a_copy(2, a, c, a_buf.at[2, a]).wait_recv()

            @pl.when(needs_a(3, r, col_next, a))
            def _():
                a_copy(3, a, col_next, a_buf.at[2, a]).start()
        each_a(one)

        @pl.when(core == 1)
        def _():
            send_b(3, row_prev2)

        def pair(a, b):
            @pl.when(needs_b(2, r, c, a, b))
            def _():
                b_copy(2, a, b, r, b_buf.at[2, a, b]).wait_recv()

                @pl.when(core == 1)
                def _():
                    hand_b(a, b).start()
        each_ab(pair)

    lax.fori_loop(0, FRONTS + 1, front, 0)

    def drain_a(a):
        for s, col in ((0, col_prev), (2, col_next), (3, col_next)):
            @pl.when(needs_a(s, r, col, a))
            def _(s=s, col=col):
                a_copy(s, a, col, a_in.at[a]).wait_send()
    each_a(drain_a)

    def drain_b(a, b):
        for s, row in ((0, row_next), (2, row_prev)):
            @pl.when(needs_b(s, row, c, a, b))
            def _(s=s, row=row):
                b_copy(s, a, b, row, b_in.at[0, b]).wait_send()

        @pl.when((core == 1) & needs_b(3, row_prev2, c, a, b))
        def _():
            b_copy(3, a, b, row_prev2, b_in.at[0, b]).wait_send()

        @pl.when((core == 1) & needs_b(2, r, c, a, b))
        def _():
            hand_b(a, b).wait_send()
        pltpu.make_async_copy(w.at[a, b], out.at[a, b], out_sem.at[a, b]).wait()
    each_ab(drain_b)

    def drain_x(s, carry):
        for q in range(PIECES):
            collect(col_route(s, q)[1])
            for a in range(2):
                collect(row_route(s, a, q)[1])
        return carry
    lax.fori_loop(0, FRONTS, drain_x, 0)


def shards(n_row, n_col, upper_a, upper_b, right_side, a_bases, b_bases, a_values, b_values):
    nb = upper_a.shape[1]
    bf16, f32 = jnp.bfloat16, jnp.float32
    b_tiles = jnp.transpose(upper_b, (0, 2, 1, 3))
    c_tiles = jnp.transpose(right_side, (0, 2, 1, 3))
    dma = pltpu.SemaphoreType.DMA
    solved = pl.pallas_call(
        functools.partial(plan, nb, n_row, n_col),
        out_shape=jax.ShapeDtypeStruct((2, 2, nb, nb), f32),
        in_specs=[pl.BlockSpec(memory_space=pl.ANY)] * 7,
        out_specs=pl.BlockSpec(memory_space=pl.ANY),
        scratch_shapes=[
            pltpu.VMEM((FRONTS, 2, nb, nb), bf16),
            pltpu.VMEM((FRONTS, 2, 2, nb, nb), bf16),
            pltpu.VMEM((FRONTS, nb, nb), bf16),
            pltpu.VMEM((FRONTS, 2, nb, nb), bf16),
            pltpu.VMEM((2, 2, nb, nb), f32),
            pltpu.VMEM((2, 2, nb, nb), bf16),
            pltpu.VMEM((nb, nb), bf16),
            pltpu.VMEM((nb, nb), bf16),
            pltpu.VMEM((nb, nb), bf16),
            pltpu.VMEM((nb, nb), f32),
            pltpu.VMEM((2, nb, nb), bf16),
            pltpu.VMEM((1, nb), f32),
            pltpu.VMEM((1, nb), f32),
            dma((5,)),
            dma((2, 2)),
            dma((FRONTS, 2)),
            dma((FRONTS, 2, 2)),
            dma((FRONTS, 2)),
            dma((FRONTS, 2, 2)),
            dma((FRONTS, PIECES, 3)),
            dma((FRONTS, 2, PIECES, 5)),
            dma((FRONTS, PIECES)),
            dma((FRONTS, 2, PIECES)),
        ],
        compiler_params=pltpu.CompilerParams(
            collective_id=0, has_side_effects=True, vmem_limit_bytes=60 * 1024 * 1024
        ),
    )(upper_a, b_tiles, c_tiles, a_bases, b_bases, a_values[:, None, :], b_values[:, None, :])
    return jnp.transpose(solved, (0, 2, 1, 3))


def solution(mesh):
    return jax.shard_map(
        functools.partial(shards, mesh.shape["row"], mesh.shape["col"]),
        mesh=mesh,
        in_specs=(
            P(None, "row", "col"),
            P(None, "row", None, "col"),
            P(None, "row", None, "col"),
            P(None, "row", None),
            P(None, "col", None),
            P(None, "row"),
            P(None, "col"),
        ),
        out_specs=P(None, "row", None, "col"),
        check_vma=False,
    )
```

```python
import functools

import jax
import jax.numpy as jnp
from jax import lax
from jax.experimental import pallas as pl
from jax.experimental.pallas import tpu as pltpu
from jax.sharding import PartitionSpec as P

MESH = pl.DeviceIdType.MESH
FRONTS = 4
RING = 4
PIECES = 4


def plan(nb, n_row, n_col, a_in, b_in, c_in, qa_in, qb_in, av_in, bv_in, out,
         a_buf, b_buf, xc, xr, w, c_buf, qa, qat, qb, inv, half, av, bv,
         local_sem, out_sem, a_send, b_send, a_recv, b_recv, xc_send, xr_send, xc_recv, xr_recv):
    rows = nb // PIECES
    r = lax.axis_index("row")
    c = lax.axis_index("col")
    y, core = r // 2, r % 2
    x, z = c // RING, c % RING
    mod = lax.rem

    def row_of(yy, kk):
        return mod(yy + 2 * RING, RING) * 2 + kk

    def col_of(xx, zz):
        return mod(xx + 2 * RING, RING) * RING + mod(zz + 2 * RING, RING)

    col_next = mod(c + 1, n_col)
    col_prev = mod(c + n_col - 1, n_col)
    col_next2 = mod(c + 2, n_col)
    col_prev2 = mod(c + n_col - 2, n_col)

    shift = mod(c - r + 1 + n_col, n_col)
    turn = mod(shift, 8)
    a_own = shift // 8
    l_own = r + 8 * a_own - 1 + turn
    b_own = jnp.where(l_own >= n_col, 1, 0)
    solves = (turn < FRONTS) & (l_own >= 0)
    turn = jnp.where(solves, turn, 99)

    def remote(src, dst, send, recv, row, col):
        return pltpu.make_async_remote_copy(
            src_ref=src, dst_ref=dst, send_sem=send, recv_sem=recv,
            device_id=(row, col), device_id_type=MESH)

    def k_of(s, col):
        return mod(col + 1 - s + n_col, n_col)

    def has_col(s, col):
        return jnp.logical_not((s == 0) & (col == n_col - 1))

    def needs_a(s, row, col, a):
        return has_col(s, col) & (row + 8 * a < k_of(s, col))

    def needs_b(s, row, col, a, b):
        l = row + 8 * a - 1 + s
        return (l >= 0) & (l < col + n_col * b)

    def a_copy(s, a, col, src):
        return remote(src, a_buf.at[s, a], a_send.at[s, a], a_recv.at[s, a], r, col)

    def b_copy(s, a, b, row, src):
        return remote(src, b_buf.at[s, a, b], b_send.at[s, a, b], b_recv.at[s, a, b], row, c)

    def hand_b(a, b):
        return remote(b_buf.at[2, a, b], b_buf.at[3, a, b], b_send.at[1, a, b], b_recv.at[3, a, b], partner, c)

    def each_a(fn):
        for a in range(2):
            fn(a)

    def each_ab(fn):
        for a in range(2):
            for b in range(2):
                fn(a, b)

    def send_a(s, col, tiles=(0, 1)):
        for a in tiles:
            @pl.when(needs_a(s, r, col, a))
            def _(a=a):
                a_copy(s, a, col, a_in.at[a]).start()

    def send_b(s, row):
        def one(a, b):
            @pl.when(needs_b(s, row, c, a, b))
            def _():
                l4 = (row + 8 * a - 1 + s) // 8
                b_copy(s, a, b, row, b_in.at[l4, b]).start()
        each_ab(one)

    row_next = mod(r + 1, n_row)
    row_prev = mod(r + n_row - 1, n_row)
    row_prev2 = mod(r + n_row - 2, n_row)
    partner = y * 2 + 1 - core

    def piece_of(q):
        return pl.ds(pl.multiple_of(q * rows, rows), rows), 1 - 2 * mod(q, 2)

    def col_route(s, q):
        piece, g = piece_of(q)
        k = k_of(s, c)
        rr = mod(k, 8)
        ry = rr // 2
        valid = has_col(s, c)
        root = valid & (r == rr)
        oy = mod((y - ry) * g + RING, RING)
        relay = valid & (oy != 0) & (core == 1)

        def copy(n, row):
            return remote(xc.at[s, piece], xc.at[s, piece], xc_send.at[s, q, n], xc_recv.at[s, q], row, c)

        sends = [
            (root | (relay & (oy == 1)), copy(0, row_of(y + g, 1))),
            (root, copy(1, row_of(y - g, 1))),
            (root | relay, copy(2, partner)),
        ]
        return valid & (r != rr), sends

    def row_route(s, a, q):
        piece, g = piece_of(q)
        l = r + 8 * a - 1 + s
        valid = l >= 0
        lc = mod(l + n_col, n_col)
        rx, rz = lc // RING, lc % RING
        root = valid & (c == lc)
        oz = mod((z - rz) * g + RING, RING)
        ox = mod((x - rx) * g + RING, RING)
        jump = rz == RING - 1
        jump_to = mod(lc + 1, n_col)

        def copy(n, col):
            return remote(xr.at[s, a, piece], xr.at[s, a, piece], xr_send.at[s, a, q, n], xr_recv.at[s, a, q], r, col)

        def step(when, n, col):
            return valid & when & jnp.logical_not(jump & (col == jump_to)), copy(n, col)

        turned = core > 1
        one, two = jnp.where(turned, ox, oz), jnp.where(turned, oz, ox)
        z_forth, z_back = col_of(x, z + g), col_of(x, z - g)
        x_forth, x_back = col_of(x + g, z), col_of(x - g, z)
        sends = [
            (root & jump, copy(4, col_next)),
            step((two == 0) & ((one == 0) | (one == 1)), 0, jnp.where(turned, x_forth, z_forth)),
            step((two == 0) & (one == 0), 1, jnp.where(turned, x_back, z_back)),
            step((two == 0) | (two == 1), 2, jnp.where(turned, z_forth, x_forth)),
            step(two == 0, 3, jnp.where(turned, z_back, x_back)),
        ]
        return valid & (c != lc), sends

    def launch(sends):
        for when, copy in sends:
            @pl.when(when)
            def _(copy=copy):
                copy.start()

    def collect(sends):
        for when, copy in sends:
            @pl.when(when)
            def _(copy=copy):
                copy.wait_send()

    def take(route):
        arrives, sends = route

        @pl.when(arrives)
        def _():
            sends[-1][1].wait_recv()
            launch(sends)

    def each_piece(fn):
        def body(q, carry):
            fn(q)
            return carry
        lax.fori_loop(0, PIECES, body, 0)

    f32 = jnp.float32

    def matmul(p, q):
        return jnp.dot(p, q, preferred_element_type=f32)

    def update_col(s, a, b):
        i, j = r + 8 * a, c + n_col * b
        k = j + 1 - s

        @pl.when((k >= 0) & (k < n_col) & (i < k))
        def _():
            a_copy(s, a, c, a_buf.at[s, a]).wait_recv()
            w[a, b] = w[a, b] - matmul(a_buf[s, a], xc[s])

    def update_row(s, a, b):
        @pl.when(needs_b(s, r, c, a, b))
        def _():
            @pl.when(s != 2)
            def _():
                b_copy(s, a, b, r, b_buf.at[s, a, b]).wait_recv()
            w[a, b] = w[a, b] - matmul(xr[s, a], b_buf[s, a, b])

    def hand_on():
        def one(a, b):
            @pl.when(needs_b(2, r, c, a, b))
            def _():
                b_copy(2, a, b, r, b_buf.at[2, a, b]).wait_recv()

                @pl.when(core == 1)
                def _():
                    hand_b(a, b).start()
        each_ab(one)

    def solve(s):
        half[0] = w[a_own, b_own].astype(jnp.bfloat16)
        half[1] = matmul(qat[...], half[0]).astype(jnp.bfloat16)
        half[0] = (matmul(half[1], qb[...]) * inv[...]).astype(jnp.bfloat16)

        def finish(q):
            piece, _ = piece_of(q)
            left = matmul(qa[piece, :], half[0]).astype(jnp.bfloat16)
            tile = lax.dot_general(left, qb[...], (((1,), (1,)), ((), ())), preferred_element_type=f32)
            tile = tile.astype(jnp.bfloat16)
            xr[s, a_own, piece, :] = tile
            xc[s, piece, :] = tile
            w[a_own, b_own, piece, :] = tile.astype(f32)
            launch(row_route(s, a_own, q)[1])
            launch(col_route(s, q)[1])
        each_piece(finish)

    barrier = pltpu.get_barrier_semaphore()
    friends = [(partner, c), (r, col_next), (r, col_prev), (r, col_next2), (r, col_prev2)]
    for d in (1, -1):
        friends += [(row_of(y + d, 0), c), (row_of(y + d, 1), c), (r, col_of(x, z + d)), (r, col_of(x + d, z))]
    for friend in friends:
        pl.semaphore_signal(barrier, inc=1, device_id=friend, device_id_type=MESH)

    loads = [
        pltpu.make_async_copy(c_in, c_buf, local_sem.at[0]),
        pltpu.make_async_copy(qa_in.at[a_own], qa, local_sem.at[1]),
        pltpu.make_async_copy(qb_in.at[b_own], qb, local_sem.at[2]),
        pltpu.make_async_copy(av_in, av, local_sem.at[3]),
        pltpu.make_async_copy(bv_in, bv, local_sem.at[4]),
    ]
    for load in loads:
        load.start()

    def local_a(a):
        return pltpu.make_async_copy(a_in.at[a], a_buf.at[1, a], a_recv.at[1, a])

    def local_b(a, b):
        return pltpu.make_async_copy(b_in.at[a, b], b_buf.at[1, a, b], b_recv.at[1, a, b])

    each_a(lambda a: pl.when(needs_a(1, r, c, a))(lambda: local_a(a).start()))
    each_ab(lambda a, b: pl.when(needs_b(1, r, c, a, b))(lambda: local_b(a, b).start()))

    pl.semaphore_wait(barrier, len(friends))
    for load in loads:
        load.wait()

    @pl.when(solves)
    def _():
        qat[...] = qa[...].T
        down = jnp.broadcast_to(jnp.where(a_own == 0, av[0:1, :], av[1:2, :]), (128, nb)).T
        across = jnp.where(b_own == 0, bv[0:1, :], bv[1:2, :])
        for n in range(nb // 128):
            lanes = pl.ds(n * 128, 128)
            inv[:, lanes] = 1.0 / (down + across[:, n * 128:n * 128 + 128])

    def load_w(t, carry):
        w[t // 2, t % 2] = c_buf[t // 2, t % 2].astype(f32)
        return carry
    lax.fori_loop(0, 4, load_w, 0)

    def near(s):
        l = mod(r - 1 + s + n_col, n_col)
        gap = mod(x - l // RING + RING, RING)
        return jnp.where((gap == 0) | (gap == 1), 0, 1), ((gap == 0) | (gap == 2))

    def far(p):
        a_first, _ = near(p)
        each_piece(lambda q: take(row_route(p, 1 - a_first, q)))

    def settled(p, a, b):
        return solves & (turn > p) & (a == a_own) & (b == b_own)

    def put_off(p, a):
        a_first, centre = near(p)
        return centre & (a != a_first)

    def stream(t):
        h = mod(shift, 8)

        def when(point, send):
            pl.when(t == point)(send)

        when(jnp.where(h == 7, 1, 0), lambda: send_a(0, col_prev))
        when(jnp.where((core == 1) & ((h == 5) | (h == 6)), 1, 0), lambda: send_b(0, row_next))
        when(jnp.where(h == 1, 1, 0), lambda: send_a(2, col_next))
        when(jnp.where((core == 0) & (h == 1), 1, 0), lambda: send_b(2, row_prev))
        late = (core == 0) & (z > 1)
        when(jnp.where(late, 2, jnp.where(h == 1, 1, jnp.where(h == 2, 2, 0))), lambda: send_a(3, col_next2, (0,)))
        when(jnp.where(late, 3, jnp.where(h == 1, 1, jnp.where(h == 2, 2, 0))), lambda: send_a(3, col_next2, (1,)))

        @pl.when(core == 1)
        def _():
            when(jnp.where(h == 0, 2, jnp.where(h == 1, 3, 0)), lambda: send_b(3, row_prev2))

    def front(t, carry):
        s = t - 1

        @pl.when(t > 0)
        def _():
            a, centre = near(s)
            ahead = solves & (turn >= t)

            @pl.when(centre | ahead)
            def _():
                def both(q):
                    take(row_route(s, a, q))
                    take(col_route(s, q))
                each_piece(both)

            @pl.when(jnp.logical_not(centre | ahead))
            def _():
                each_piece(lambda q: take(col_route(s, q)))

                def both(q):
                    take(row_route(s, a, q))
                    take(row_route(s, 1 - a, q))
                each_piece(both)

            pl.when((t == 3) & (turn == 3))(hand_on)

            @pl.when(ahead)
            def _():
                update_col(s, a_own, b_own)
                update_row(s, a_own, b_own)

        @pl.when(turn == t)
        def _():
            solve(t)

            def catch_up(p, carry):
                pl.when(jnp.logical_not(near(p)[1]))(lambda: far(p))
                return carry
            lax.fori_loop(0, t, catch_up, 0)

        stream(t)
        pl.when((t == 3) & (turn != 3))(hand_on)

        def rest(m, carry):
            p = jnp.where(t == FRONTS, jnp.where(m < 2, 2 * m, FRONTS - 1), 1)

            def one(n, carry):
                a, b = n // 2, mod(n, 2)

                @pl.when(jnp.logical_not(settled(p, a, b)))
                def _():
                    update_col(p, a, b)
                    pl.when(jnp.logical_not(put_off(p, a)))(lambda: update_row(p, a, b))
                return carry
            return lax.fori_loop(0, 4, one, carry)
        lax.fori_loop(0, jnp.where(t == FRONTS, 3, jnp.where(t == 3, 1, 0)), rest, 0)
        return carry

    lax.fori_loop(0, FRONTS + 1, front, 0)

    def last(n, carry):
        a_first, _ = near(FRONTS - 1)
        a = jnp.where(n < 2, a_first, 1 - a_first)
        b = mod(n, 2)

        def one(p, carry):
            @pl.when(put_off(p, a))
            def _():
                pl.when(b == 0)(lambda: far(p))
                pl.when(jnp.logical_not(settled(p, a, b)))(lambda: update_row(p, a, b))
            return carry
        lax.fori_loop(0, FRONTS, one, 0)
        pltpu.make_async_copy(w.at[a, b], out.at[a, b], out_sem.at[a, b]).start()
        return carry
    lax.fori_loop(0, 4, last, 0)

    def drain_a(a):
        for s, col in ((0, col_prev), (2, col_next), (3, col_next2)):
            @pl.when(needs_a(s, r, col, a))
            def _(s=s, col=col):
                a_copy(s, a, col, a_in.at[a]).wait_send()
    each_a(drain_a)

    def drain_b(a, b):
        for s, row in ((0, row_next), (2, row_prev)):
            @pl.when(needs_b(s, row, c, a, b))
            def _(s=s, row=row):
                b_copy(s, a, b, row, b_in.at[0, b]).wait_send()

        @pl.when((core == 1) & needs_b(3, row_prev2, c, a, b))
        def _():
            b_copy(3, a, b, row_prev2, b_in.at[0, b]).wait_send()

        @pl.when((core == 1) & needs_b(2, r, c, a, b))
        def _():
            hand_b(a, b).wait_send()
        pltpu.make_async_copy(w.at[a, b], out.at[a, b], out_sem.at[a, b]).wait()
    each_ab(drain_b)

    def drain_x(s, carry):
        def one(q):
            collect(col_route(s, q)[1])
            for a in range(2):
                collect(row_route(s, a, q)[1])
        each_piece(one)
        return carry
    lax.fori_loop(0, FRONTS, drain_x, 0)


def shards(n_row, n_col, upper_a, upper_b, right_side, a_bases, b_bases, a_values, b_values):
    nb = upper_a.shape[1]
    bf16, f32 = jnp.bfloat16, jnp.float32
    b_tiles = jnp.transpose(upper_b, (0, 2, 1, 3))
    c_tiles = jnp.transpose(right_side, (0, 2, 1, 3))
    dma = pltpu.SemaphoreType.DMA
    solved = pl.pallas_call(
        functools.partial(plan, nb, n_row, n_col),
        out_shape=jax.ShapeDtypeStruct((2, 2, nb, nb), f32),
        in_specs=[pl.BlockSpec(memory_space=pl.ANY)] * 7,
        out_specs=pl.BlockSpec(memory_space=pl.ANY),
        scratch_shapes=[
            pltpu.VMEM((FRONTS, 2, nb, nb), bf16),
            pltpu.VMEM((FRONTS, 2, 2, nb, nb), bf16),
            pltpu.VMEM((FRONTS, nb, nb), bf16),
            pltpu.VMEM((FRONTS, 2, nb, nb), bf16),
            pltpu.VMEM((2, 2, nb, nb), f32),
            pltpu.VMEM((2, 2, nb, nb), bf16),
            pltpu.VMEM((nb, nb), bf16),
            pltpu.VMEM((nb, nb), bf16),
            pltpu.VMEM((nb, nb), bf16),
            pltpu.VMEM((nb, nb), f32),
            pltpu.VMEM((2, nb, nb), bf16),
            pltpu.VMEM((2, nb), f32),
            pltpu.VMEM((2, nb), f32),
            dma((5,)),
            dma((2, 2)),
            dma((FRONTS, 2)),
            dma((FRONTS, 2, 2)),
            dma((FRONTS, 2)),
            dma((FRONTS, 2, 2)),
            dma((FRONTS, PIECES, 3)),
            dma((FRONTS, 2, PIECES, 5)),
            dma((FRONTS, PIECES)),
            dma((FRONTS, 2, PIECES)),
        ],
        compiler_params=pltpu.CompilerParams(
            collective_id=0, has_side_effects=True, vmem_limit_bytes=60 * 1024 * 1024
        ),
    )(upper_a, b_tiles, c_tiles, a_bases, b_bases, a_values, b_values)
    return jnp.transpose(solved, (0, 2, 1, 3))


def solution(mesh):
    return jax.shard_map(
        functools.partial(shards, mesh.shape["row"], mesh.shape["col"]),
        mesh=mesh,
        in_specs=(
            P(None, "row", "col"),
            P(None, "row", None, "col"),
            P(None, "row", None, "col"),
            P(None, "row", None),
            P(None, "col", None),
            P(None, "row"),
            P(None, "col"),
        ),
        out_specs=P(None, "row", None, "col"),
        check_vma=False,
    )
```

```python
import functools

import jax
import jax.numpy as jnp
from jax import lax
from jax.experimental import pallas as pl
from jax.experimental.pallas import tpu as pltpu
from jax.sharding import PartitionSpec as P

MESH = pl.DeviceIdType.MESH
FRONTS = 4
RING = 4
PIECES = 2


def plan(nb, n_row, n_col, a_in, b_in, c_in, qa_in, qb_in, av_in, bv_in, out,
         a_buf, b_buf, xc, xr, w, c_buf, qa, qat, qb, inv, half, av, bv,
         local_sem, out_sem, a_send, b_send, a_recv, b_recv, xc_send, xr_send, xc_recv, xr_recv):
    rows = nb // PIECES
    r = lax.axis_index("row")
    c = lax.axis_index("col")
    y, core = r // 2, r % 2
    x, z = c // RING, c % RING
    mod = lax.rem

    def row_of(yy, kk):
        return mod(yy + 2 * RING, RING) * 2 + kk

    def col_of(xx, zz):
        return mod(xx + 2 * RING, RING) * RING + mod(zz + 2 * RING, RING)

    col_next = mod(c + 1, n_col)
    col_prev = mod(c + n_col - 1, n_col)
    col_next2 = mod(c + 2, n_col)
    col_prev2 = mod(c + n_col - 2, n_col)

    shift = mod(c - r + 1 + n_col, n_col)
    turn = mod(shift, 8)
    a_own = shift // 8
    l_own = r + 8 * a_own - 1 + turn
    b_own = jnp.where(l_own >= n_col, 1, 0)
    solves = (turn < FRONTS) & (l_own >= 0)
    turn = jnp.where(solves, turn, 99)
    leaps = solves & (z == RING - 1)

    def remote(src, dst, send, recv, row, col):
        return pltpu.make_async_remote_copy(
            src_ref=src, dst_ref=dst, send_sem=send, recv_sem=recv,
            device_id=(row, col), device_id_type=MESH)

    def k_of(s, col):
        return mod(col + 1 - s + n_col, n_col)

    def has_col(s, col):
        return jnp.logical_not((s == 0) & (col == n_col - 1))

    def needs_a(s, row, col, a):
        return has_col(s, col) & (row + 8 * a < k_of(s, col))

    def needs_b(s, row, col, a, b):
        l = row + 8 * a - 1 + s
        return (l >= 0) & (l < col + n_col * b)

    def a_copy(s, a, col, src):
        return remote(src, a_buf.at[s, a], a_send.at[s, a], a_recv.at[s, a], r, col)

    def b_copy(s, a, b, row, src):
        return remote(src, b_buf.at[s, a, b], b_send.at[s, a, b], b_recv.at[s, a, b], row, c)

    def hand_b(a, b):
        return remote(b_buf.at[2, a, b], b_buf.at[3, a, b], b_send.at[1, a, b], b_recv.at[3, a, b], partner, c)

    def each_a(fn):
        for a in range(2):
            fn(a)

    def each_ab(fn):
        for a in range(2):
            for b in range(2):
                fn(a, b)

    def send_a(s, col, tiles=(0, 1)):
        for a in tiles:
            @pl.when(needs_a(s, r, col, a))
            def _(a=a):
                a_copy(s, a, col, a_in.at[a]).start()

    def send_b(s, row):
        def one(a, b):
            @pl.when(needs_b(s, row, c, a, b))
            def _():
                l4 = (row + 8 * a - 1 + s) // 8
                b_copy(s, a, b, row, b_in.at[l4, b]).start()
        each_ab(one)

    row_next = mod(r + 1, n_row)
    row_prev = mod(r + n_row - 1, n_row)
    row_prev2 = mod(r + n_row - 2, n_row)
    partner = y * 2 + 1 - core

    def piece_of(q):
        return pl.ds(pl.multiple_of(q * rows, rows), rows), 1 - 2 * mod(q, 2)

    def col_route(s, q):
        piece, _ = piece_of(q)
        k = k_of(s, c)
        rr = mod(k, 8)
        ry = rr // 2
        valid = has_col(s, c)
        root = valid & (r == rr)
        oy = mod(y - ry + RING, RING)
        lands = valid & jnp.where(oy == RING - 1, core == 1, (oy != 0) & (core == 0))

        def copy(n, row):
            return remote(xc.at[s, piece], xc.at[s, piece], xc_send.at[s, q, n], xc_recv.at[s, q], row, c)

        sends = [
            (root, copy(1, row_of(y - 1, 1))),
            (root | lands, copy(2, partner)),
            (root | (lands & (oy == 1)), copy(0, row_of(y + 1, 0))),
        ]
        return valid & (r != rr), sends

    def row_route(s, a, q):
        piece, g = piece_of(q)
        l = r + 8 * a - 1 + s
        valid = l >= 0
        lc = mod(l + n_col, n_col)
        rx, rz = lc // RING, lc % RING
        root = valid & (c == lc)
        oz = mod((z - rz) * g + RING, RING)
        ox = mod((x - rx) * g + RING, RING)
        jump = rz == RING - 1
        jump_to = mod(lc + 1, n_col)

        def copy(n, col):
            return remote(xr.at[s, a, piece], xr.at[s, a, piece], xr_send.at[s, a, q, n], xr_recv.at[s, a, q], r, col)

        def step(offset, ahead, when, n, col):
            go = when & ((offset == 0) | (ahead & (offset == 1)))
            return valid & go & jnp.logical_not(jump & (col == jump_to)), copy(n, col)

        sends = [
            (root & jump, copy(4, col_next)),
            step(oz, g == 1, ox == 0, 0, col_of(x, z + 1)),
            step(oz, g == -1, ox == 0, 1, col_of(x, z - 1)),
            step(ox, g == 1, valid, 2, col_of(x + 1, z)),
            step(ox, g == -1, valid, 3, col_of(x - 1, z)),
        ]
        return valid & (c != lc), sends

    def launch(sends, held=False, only=(0, 1, 2, 3, 4), hold=()):
        for n, (when, copy) in enumerate(sends):
            if n not in only:
                continue

            @pl.when(when & jnp.logical_not(held) if n in hold else when)
            def _(copy=copy):
                copy.start()

    def collect(sends):
        for when, copy in sends:
            @pl.when(when)
            def _(copy=copy):
                copy.wait_send()

    def take(route):
        arrives, sends = route

        @pl.when(arrives)
        def _():
            sends[-1][1].wait_recv()
            launch(sends)

    def each_piece(fn):
        def body(q, carry):
            fn(q)
            return carry
        lax.fori_loop(0, PIECES, body, 0)

    f32 = jnp.float32

    def matmul(p, q):
        return jnp.dot(p, q, preferred_element_type=f32)

    def update_col(s, a, b):
        i, j = r + 8 * a, c + n_col * b
        k = j + 1 - s

        @pl.when((k >= 0) & (k < n_col) & (i < k))
        def _():
            a_copy(s, a, c, a_buf.at[s, a]).wait_recv()
            w[a, b] = w[a, b] - matmul(a_buf[s, a], xc[s])

    def update_row(s, a, b):
        @pl.when(needs_b(s, r, c, a, b))
        def _():
            @pl.when(s != 2)
            def _():
                b_copy(s, a, b, r, b_buf.at[s, a, b]).wait_recv()
            w[a, b] = w[a, b] - matmul(xr[s, a], b_buf[s, a, b])

    def hand_on():
        def one(a, b):
            @pl.when(needs_b(2, r, c, a, b))
            def _():
                b_copy(2, a, b, r, b_buf.at[2, a, b]).wait_recv()

                @pl.when(core == 1)
                def _():
                    hand_b(a, b).start()
        each_ab(one)

    def solve(s):
        half[0] = w[a_own, b_own].astype(jnp.bfloat16)
        half[1] = matmul(qat[...], half[0]).astype(jnp.bfloat16)
        half[0] = (matmul(half[1], qb[...]) * inv[...]).astype(jnp.bfloat16)

        def finish(q):
            piece, _ = piece_of(q)
            left = matmul(qa[piece, :], half[0]).astype(jnp.bfloat16)
            tile = lax.dot_general(left, qb[...], (((1,), (1,)), ((), ())), preferred_element_type=f32)
            tile = tile.astype(jnp.bfloat16)
            xr[s, a_own, piece, :] = tile
            xc[s, piece, :] = tile
            w[a_own, b_own, piece, :] = tile.astype(f32)
            launch(row_route(s, a_own, q)[1], leaps, hold=(1, 3))
            launch(col_route(s, q)[1])
        each_piece(finish)

        @pl.when(leaps)
        def _():
            each_piece(lambda q: launch(row_route(s, a_own, q)[1], only=(1, 3)))

    barrier = pltpu.get_barrier_semaphore()
    friends = [(partner, c), (r, col_next), (r, col_prev), (r, col_next2), (r, col_prev2)]
    for d in (1, -1):
        friends += [(row_of(y + d, 0), c), (row_of(y + d, 1), c), (r, col_of(x, z + d)), (r, col_of(x + d, z))]
    for friend in friends:
        pl.semaphore_signal(barrier, inc=1, device_id=friend, device_id_type=MESH)

    loads = [
        pltpu.make_async_copy(c_in, c_buf, local_sem.at[0]),
        pltpu.make_async_copy(qa_in.at[a_own], qa, local_sem.at[1]),
        pltpu.make_async_copy(qb_in.at[b_own], qb, local_sem.at[2]),
        pltpu.make_async_copy(av_in, av, local_sem.at[3]),
        pltpu.make_async_copy(bv_in, bv, local_sem.at[4]),
    ]
    for load in loads:
        load.start()

    def local_a(a):
        return pltpu.make_async_copy(a_in.at[a], a_buf.at[1, a], a_recv.at[1, a])

    def local_b(a, b):
        return pltpu.make_async_copy(b_in.at[a, b], b_buf.at[1, a, b], b_recv.at[1, a, b])

    each_a(lambda a: pl.when(needs_a(1, r, c, a))(lambda: local_a(a).start()))
    each_ab(lambda a, b: pl.when(needs_b(1, r, c, a, b))(lambda: local_b(a, b).start()))

    pl.semaphore_wait(barrier, len(friends))
    for load in loads:
        load.wait()

    @pl.when(solves)
    def _():
        qat[...] = qa[...].T
        down = jnp.broadcast_to(jnp.where(a_own == 0, av[0:1, :], av[1:2, :]), (128, nb)).T
        across = jnp.where(b_own == 0, bv[0:1, :], bv[1:2, :])
        for n in range(nb // 128):
            lanes = pl.ds(n * 128, 128)
            inv[:, lanes] = 1.0 / (down + across[:, n * 128:n * 128 + 128])

    def load_w(t, carry):
        w[t // 2, t % 2] = c_buf[t // 2, t % 2].astype(f32)
        return carry
    lax.fori_loop(0, 4, load_w, 0)

    def near(s):
        l = mod(r - 1 + s + n_col, n_col)
        gap = mod(x - l // RING + RING, RING)
        return jnp.where((gap == 0) | (gap == 1), 0, 1), ((gap == 0) | (gap == 2))

    def far(p):
        a_first, _ = near(p)
        each_piece(lambda q: take(row_route(p, 1 - a_first, q)))

    def settled(p, a, b):
        return solves & (turn > p) & (a == a_own) & (b == b_own)

    def put_off(p, a):
        a_first, centre = near(p)
        return centre & (a != a_first)

    def stream(t):
        h = mod(shift, 8)

        def when(point, send):
            pl.when(t == point)(send)

        when(jnp.where(h == 7, 1, 0), lambda: send_a(0, col_prev))
        when(0, lambda: send_b(0, row_next))
        when(jnp.where(h == 1, 1, 0), lambda: send_a(2, col_next))
        when(jnp.where((core == 0) & (h == 1), 1, 0), lambda: send_b(2, row_prev))
        late = (core == 0) & (z > 1)
        when(jnp.where(late, 2, jnp.where(h == 1, 1, jnp.where(h == 2, 2, 0))), lambda: send_a(3, col_next2, (0,)))
        when(jnp.where(late, 3, jnp.where(h == 1, 1, jnp.where(h == 2, 2, 0))), lambda: send_a(3, col_next2, (1,)))

        @pl.when(core == 1)
        def _():
            when(jnp.where(h == 0, 2, jnp.where(h == 1, 3, 0)), lambda: send_b(3, row_prev2))

    def front(t, carry):
        s = t - 1

        @pl.when(t > 0)
        def _():
            a, centre = near(s)
            ahead = solves & (turn >= t)

            @pl.when(centre | ahead)
            def _():
                def both(q):
                    take(row_route(s, a, q))
                    take(col_route(s, q))
                each_piece(both)

            @pl.when(jnp.logical_not(centre | ahead))
            def _():
                each_piece(lambda q: take(col_route(s, q)))

                def both(q):
                    take(row_route(s, a, q))
                    take(row_route(s, 1 - a, q))
                each_piece(both)

            pl.when((t == 3) & (turn == 3))(hand_on)

            @pl.when(ahead)
            def _():
                update_col(s, a_own, b_own)
                update_row(s, a_own, b_own)

        @pl.when(turn == t)
        def _():
            solve(t)

            def catch_up(p, carry):
                pl.when(jnp.logical_not(near(p)[1]))(lambda: far(p))
                return carry
            lax.fori_loop(0, t, catch_up, 0)

        stream(t)
        pl.when((t == 3) & (turn != 3))(hand_on)

        def rest(m, carry):
            p = jnp.where(t == FRONTS, jnp.where(m < 2, 2 * m, FRONTS - 1), 1)

            def one(n, carry):
                a, b = n // 2, mod(n, 2)

                @pl.when(jnp.logical_not(settled(p, a, b)))
                def _():
                    update_col(p, a, b)
                    pl.when(jnp.logical_not(put_off(p, a)))(lambda: update_row(p, a, b))
                return carry
            return lax.fori_loop(0, 4, one, carry)
        lax.fori_loop(0, jnp.where(t == FRONTS, 3, jnp.where(t == 3, 1, 0)), rest, 0)
        return carry

    lax.fori_loop(0, FRONTS + 1, front, 0)

    def last(n, carry):
        a_first, _ = near(FRONTS - 1)
        a = jnp.where(n < 2, a_first, 1 - a_first)
        b = mod(n, 2)

        def one(p, carry):
            @pl.when(put_off(p, a))
            def _():
                pl.when(b == 0)(lambda: far(p))
                pl.when(jnp.logical_not(settled(p, a, b)))(lambda: update_row(p, a, b))
            return carry
        lax.fori_loop(0, FRONTS, one, 0)
        pltpu.make_async_copy(w.at[a, b], out.at[a, :, b], out_sem.at[a, b]).start()
        return carry
    lax.fori_loop(0, 4, last, 0)

    def drain_a(a):
        for s, col in ((0, col_prev), (2, col_next), (3, col_next2)):
            @pl.when(needs_a(s, r, col, a))
            def _(s=s, col=col):
                a_copy(s, a, col, a_in.at[a]).wait_send()
    each_a(drain_a)

    def drain_b(a, b):
        for s, row in ((0, row_next), (2, row_prev)):
            @pl.when(needs_b(s, row, c, a, b))
            def _(s=s, row=row):
                b_copy(s, a, b, row, b_in.at[0, b]).wait_send()

        @pl.when((core == 1) & needs_b(3, row_prev2, c, a, b))
        def _():
            b_copy(3, a, b, row_prev2, b_in.at[0, b]).wait_send()

        @pl.when((core == 1) & needs_b(2, r, c, a, b))
        def _():
            hand_b(a, b).wait_send()
        pltpu.make_async_copy(w.at[a, b], out.at[a, :, b], out_sem.at[a, b]).wait()
    each_ab(drain_b)

    def drain_x(s, carry):
        def one(q):
            collect(col_route(s, q)[1])
            for a in range(2):
                collect(row_route(s, a, q)[1])
        each_piece(one)
        return carry
    lax.fori_loop(0, FRONTS, drain_x, 0)


def shards(n_row, n_col, upper_a, upper_b, right_side, a_bases, b_bases, a_values, b_values):
    nb = upper_a.shape[1]
    bf16, f32 = jnp.bfloat16, jnp.float32
    b_tiles = jnp.transpose(upper_b[:3], (0, 2, 1, 3))
    c_tiles = jnp.transpose(right_side, (0, 2, 1, 3))
    dma = pltpu.SemaphoreType.DMA
    solved = pl.pallas_call(
        functools.partial(plan, nb, n_row, n_col),
        out_shape=jax.ShapeDtypeStruct((2, nb, 2, nb), f32),
        in_specs=[pl.BlockSpec(memory_space=pl.ANY)] * 7,
        out_specs=pl.BlockSpec(memory_space=pl.ANY),
        scratch_shapes=[
            pltpu.VMEM((FRONTS, 2, nb, nb), bf16),
            pltpu.VMEM((FRONTS, 2, 2, nb, nb), bf16),
            pltpu.VMEM((FRONTS, nb, nb), bf16),
            pltpu.VMEM((FRONTS, 2, nb, nb), bf16),
            pltpu.VMEM((2, 2, nb, nb), f32),
            pltpu.VMEM((2, 2, nb, nb), bf16),
            pltpu.VMEM((nb, nb), bf16),
            pltpu.VMEM((nb, nb), bf16),
            pltpu.VMEM((nb, nb), bf16),
            pltpu.VMEM((nb, nb), f32),
            pltpu.VMEM((2, nb, nb), bf16),
            pltpu.VMEM((2, nb), f32),
            pltpu.VMEM((2, nb), f32),
            dma((5,)),
            dma((2, 2)),
            dma((FRONTS, 2)),
            dma((FRONTS, 2, 2)),
            dma((FRONTS, 2)),
            dma((FRONTS, 2, 2)),
            dma((FRONTS, PIECES, 3)),
            dma((FRONTS, 2, PIECES, 5)),
            dma((FRONTS, PIECES)),
            dma((FRONTS, 2, PIECES)),
        ],
        compiler_params=pltpu.CompilerParams(
            collective_id=0, has_side_effects=True, vmem_limit_bytes=60 * 1024 * 1024
        ),
    )(upper_a, b_tiles, c_tiles, a_bases, b_bases, a_values, b_values)
    return solved


def solution(mesh):
    return jax.shard_map(
        functools.partial(shards, mesh.shape["row"], mesh.shape["col"]),
        mesh=mesh,
        in_specs=(
            P(None, "row", "col"),
            P(None, "row", None, "col"),
            P(None, "row", None, "col"),
            P(None, "row", None),
            P(None, "col", None),
            P(None, "row"),
            P(None, "col"),
        ),
        out_specs=P(None, "row", None, "col"),
        check_vma=False,
    )
```

```python
import functools

import jax
import jax.numpy as jnp
from jax import lax
from jax.experimental import pallas as pl
from jax.experimental.pallas import tpu as pltpu
from jax.sharding import PartitionSpec as P

MESH = pl.DeviceIdType.MESH
FRONTS = 4
RING = 4
PIECES = 2


def plan(nb, n_row, n_col, a_in, b_in, c_in, qa_in, qb_in, av_in, bv_in, out,
         a_buf, b_buf, xc, xr, w, c_buf, qa, qat, qb, inv, half, av, bv,
         local_sem, out_sem, a_send, b_send, a_recv, b_recv, xc_send, xr_send, xc_recv, xr_recv):
    rows = nb // PIECES
    r = lax.axis_index("row")
    c = lax.axis_index("col")
    y, core = r // 2, r % 2
    x, z = c // RING, c % RING
    mod = lax.rem

    def row_of(yy, kk):
        return mod(yy + 2 * RING, RING) * 2 + kk

    def col_of(xx, zz):
        return mod(xx + 2 * RING, RING) * RING + mod(zz + 2 * RING, RING)

    col_next = mod(c + 1, n_col)
    col_prev = mod(c + n_col - 1, n_col)
    col_next2 = mod(c + 2, n_col)
    col_prev2 = mod(c + n_col - 2, n_col)

    shift = mod(c - r + 1 + n_col, n_col)
    turn = mod(shift, 8)
    a_own = shift // 8
    l_own = r + 8 * a_own - 1 + turn
    b_own = jnp.where(l_own >= n_col, 1, 0)
    solves = (turn < FRONTS) & (l_own >= 0)
    turn = jnp.where(solves, turn, 99)
    leaps = solves & (z == RING - 1)

    def remote(src, dst, send, recv, row, col):
        return pltpu.make_async_remote_copy(
            src_ref=src, dst_ref=dst, send_sem=send, recv_sem=recv,
            device_id=(row, col), device_id_type=MESH)

    def k_of(s, col):
        return mod(col + 1 - s + n_col, n_col)

    def has_col(s, col):
        return jnp.logical_not((s == 0) & (col == n_col - 1))

    def needs_a(s, row, col, a):
        return has_col(s, col) & (row + 8 * a < k_of(s, col))

    def needs_b(s, row, col, a, b):
        l = row + 8 * a - 1 + s
        return (l >= 0) & (l < col + n_col * b)

    def a_copy(s, a, col, src):
        return remote(src, a_buf.at[s, a], a_send.at[s, a], a_recv.at[s, a], r, col)

    def b_copy(s, a, b, row, src):
        return remote(src, b_buf.at[s, a, b], b_send.at[s, a, b], b_recv.at[s, a, b], row, c)

    def hand_b(a, b):
        return remote(b_buf.at[2, a, b], b_buf.at[3, a, b], b_send.at[1, a, b], b_recv.at[3, a, b], partner, c)

    def each_a(fn):
        for a in range(2):
            fn(a)

    def each_ab(fn):
        for a in range(2):
            for b in range(2):
                fn(a, b)

    def send_a(s, col, tiles=(0, 1)):
        for a in tiles:
            @pl.when(needs_a(s, r, col, a))
            def _(a=a):
                a_copy(s, a, col, a_in.at[a]).start()

    def send_b(s, row):
        def one(a, b):
            @pl.when(needs_b(s, row, c, a, b))
            def _():
                l4 = (row + 8 * a - 1 + s) // 8
                b_copy(s, a, b, row, b_in.at[l4, b]).start()
        each_ab(one)

    row_next = mod(r + 1, n_row)
    row_prev = mod(r + n_row - 1, n_row)
    row_prev2 = mod(r + n_row - 2, n_row)
    partner = y * 2 + 1 - core

    def piece_of(q):
        return pl.ds(pl.multiple_of(q * rows, rows), rows), 1 - 2 * mod(q, 2)

    def col_route(s, q):
        piece, _ = piece_of(q)
        k = k_of(s, c)
        rr = mod(k, 8)
        ry = rr // 2
        valid = has_col(s, c)
        root = valid & (r == rr)
        oy = mod(y - ry + RING, RING)
        lands = valid & jnp.where(oy == RING - 1, core == 1, (oy != 0) & (core == 0))

        def copy(n, row):
            return remote(xc.at[s, piece], xc.at[s, piece], xc_send.at[s, q, n], xc_recv.at[s, q], row, c)

        sends = [
            (root, copy(1, row_of(y - 1, 1))),
            (root | lands, copy(2, partner)),
            (root | (lands & (oy == 1)), copy(0, row_of(y + 1, 0))),
        ]
        return valid & (r != rr), sends

    def row_route(s, a, q):
        piece, g = piece_of(q)
        l = r + 8 * a - 1 + s
        valid = l >= 0
        lc = mod(l + n_col, n_col)
        rx, rz = lc // RING, lc % RING
        root = valid & (c == lc)
        oz = mod((z - rz) * g + RING, RING)
        ox = mod((x - rx) * g + RING, RING)
        jump = rz == RING - 1
        jump_to = mod(lc + 1, n_col)

        def copy(n, col):
            return remote(xr.at[s, a, piece], xr.at[s, a, piece], xr_send.at[s, a, q, n], xr_recv.at[s, a, q], r, col)

        def step(offset, ahead, when, n, col):
            go = when & ((offset == 0) | (ahead & (offset == 1)))
            return valid & go & jnp.logical_not(jump & (col == jump_to)), copy(n, col)

        sends = [
            (root & jump, copy(4, col_next)),
            step(oz, g == 1, ox == 0, 0, col_of(x, z + 1)),
            step(oz, g == -1, ox == 0, 1, col_of(x, z - 1)),
            step(ox, g == 1, valid, 2, col_of(x + 1, z)),
            step(ox, g == -1, valid, 3, col_of(x - 1, z)),
        ]
        return valid & (c != lc), sends

    def launch(sends, held=False, only=(0, 1, 2, 3, 4), hold=()):
        for n, (when, copy) in enumerate(sends):
            if n not in only:
                continue

            @pl.when(when & jnp.logical_not(held) if n in hold else when)
            def _(copy=copy):
                copy.start()

    def collect(sends):
        for when, copy in sends:
            @pl.when(when)
            def _(copy=copy):
                copy.wait_send()

    def take(route):
        arrives, sends = route

        @pl.when(arrives)
        def _():
            sends[-1][1].wait_recv()
            launch(sends)

    def each_piece(fn):
        def body(q, carry):
            fn(q)
            return carry
        lax.fori_loop(0, PIECES, body, 0)

    f32 = jnp.float32

    def matmul(p, q):
        return jnp.dot(p, q, preferred_element_type=f32)

    def update_col(s, a, b):
        i, j = r + 8 * a, c + n_col * b
        k = j + 1 - s

        @pl.when((k >= 0) & (k < n_col) & (i < k))
        def _():
            @pl.when(s != 2)
            def _():
                a_copy(s, a, c, a_buf.at[s, a]).wait_recv()
            w[a, b] = w[a, b] - matmul(a_buf[s, a], xc[s])

    def update_row(s, a, b):
        @pl.when(needs_b(s, r, c, a, b))
        def _():
            @pl.when(s != 2)
            def _():
                b_copy(s, a, b, r, b_buf.at[s, a, b]).wait_recv()
            w[a, b] = w[a, b] - matmul(xr[s, a], b_buf[s, a, b])

    def direct_a(a):
        return remote(a_in.at[a], a_buf.at[3, a], a_send.at[1, a], a_recv.at[3, a], r, col_next2)

    def leave_a(go):
        for a in range(2):
            @pl.when((mod(shift, 8) == 2) & needs_a(3, r, col_next2, a))
            def _(a=a):
                go(direct_a(a))

    def relay_a():
        for a in range(2):
            @pl.when(needs_a(3, r, col_next, a) & (mod(shift, 8) != 3))
            def _(a=a):
                a_copy(3, a, col_next, a_buf.at[2, a]).start()

    def hand_on():
        for a in range(2):
            @pl.when(needs_a(2, r, c, a))
            def _(a=a):
                a_copy(2, a, c, a_buf.at[2, a]).wait_recv()

        def one(a, b):
            @pl.when(needs_b(2, r, c, a, b))
            def _():
                b_copy(2, a, b, r, b_buf.at[2, a, b]).wait_recv()

                @pl.when(core == 1)
                def _():
                    hand_b(a, b).start()
        each_ab(one)

    def solve(s):
        half[0] = w[a_own, b_own].astype(jnp.bfloat16)
        half[1] = matmul(qat[...], half[0]).astype(jnp.bfloat16)
        half[0] = (matmul(half[1], qb[...]) * inv[...]).astype(jnp.bfloat16)

        def finish(q):
            piece, _ = piece_of(q)
            left = matmul(qa[piece, :], half[0]).astype(jnp.bfloat16)
            tile = lax.dot_general(left, qb[...], (((1,), (1,)), ((), ())), preferred_element_type=f32)
            tile = tile.astype(jnp.bfloat16)
            xr[s, a_own, piece, :] = tile
            xc[s, piece, :] = tile
            w[a_own, b_own, piece, :] = tile.astype(f32)
            launch(row_route(s, a_own, q)[1], leaps, hold=(1, 3))
            launch(col_route(s, q)[1])
        each_piece(finish)

        @pl.when(leaps)
        def _():
            each_piece(lambda q: launch(row_route(s, a_own, q)[1], only=(1, 3)))

    barrier = pltpu.get_barrier_semaphore()
    friends = [(partner, c), (r, col_next), (r, col_prev), (r, col_next2), (r, col_prev2)]
    for d in (1, -1):
        friends += [(row_of(y + d, 0), c), (row_of(y + d, 1), c), (r, col_of(x, z + d)), (r, col_of(x + d, z))]
    for friend in friends:
        pl.semaphore_signal(barrier, inc=1, device_id=friend, device_id_type=MESH)

    loads = [
        pltpu.make_async_copy(c_in, c_buf, local_sem.at[0]),
        pltpu.make_async_copy(qa_in.at[a_own], qa, local_sem.at[1]),
        pltpu.make_async_copy(qb_in.at[b_own], qb, local_sem.at[2]),
        pltpu.make_async_copy(av_in, av, local_sem.at[3]),
        pltpu.make_async_copy(bv_in, bv, local_sem.at[4]),
    ]
    for load in loads:
        load.start()

    def local_a(a):
        return pltpu.make_async_copy(a_in.at[a], a_buf.at[1, a], a_recv.at[1, a])

    def local_b(a, b):
        return pltpu.make_async_copy(b_in.at[a, b], b_buf.at[1, a, b], b_recv.at[1, a, b])

    each_a(lambda a: pl.when(needs_a(1, r, c, a))(lambda: local_a(a).start()))
    each_ab(lambda a, b: pl.when(needs_b(1, r, c, a, b))(lambda: local_b(a, b).start()))

    pl.semaphore_wait(barrier, len(friends))
    for load in loads:
        load.wait()

    @pl.when(solves)
    def _():
        qat[...] = qa[...].T
        down = jnp.broadcast_to(jnp.where(a_own == 0, av[0:1, :], av[1:2, :]), (128, nb)).T
        across = jnp.where(b_own == 0, bv[0:1, :], bv[1:2, :])
        for n in range(nb // 128):
            lanes = pl.ds(n * 128, 128)
            inv[:, lanes] = 1.0 / (down + across[:, n * 128:n * 128 + 128])

    def load_w(t, carry):
        w[t // 2, t % 2] = c_buf[t // 2, t % 2].astype(f32)
        return carry
    lax.fori_loop(0, 4, load_w, 0)

    def near(s):
        l = mod(r - 1 + s + n_col, n_col)
        gap = mod(x - l // RING + RING, RING)
        return jnp.where((gap == 0) | (gap == 1), 0, 1), ((gap == 0) | (gap == 2))

    def far(p):
        a_first, _ = near(p)
        each_piece(lambda q: take(row_route(p, 1 - a_first, q)))

    def settled(p, a, b):
        return solves & (turn > p) & (a == a_own) & (b == b_own)

    def put_off(p, a):
        a_first, centre = near(p)
        return centre & (a != a_first)

    def stream(t):
        h = mod(shift, 8)

        def when(point, send):
            pl.when(t == point)(send)

        when(jnp.where(h == 7, 1, 0), lambda: send_a(0, col_prev))
        when(0, lambda: send_b(0, row_next))
        when(jnp.where(h == 1, 1, 0), lambda: send_a(2, col_next))
        when(jnp.where((core == 0) & (h == 1), 1, 0), lambda: send_b(2, row_prev))
        when(2, lambda: leave_a(lambda copy: copy.start()))

        @pl.when(core == 1)
        def _():
            when(jnp.where(h == 0, 2, jnp.where(h == 1, 3, 0)), lambda: send_b(3, row_prev2))

    def front(t, carry):
        s = t - 1

        @pl.when(t > 0)
        def _():
            a, centre = near(s)
            ahead = solves & (turn >= t)

            @pl.when(centre | ahead)
            def _():
                def both(q):
                    take(row_route(s, a, q))
                    take(col_route(s, q))
                each_piece(both)

            @pl.when(jnp.logical_not(centre | ahead))
            def _():
                each_piece(lambda q: take(col_route(s, q)))

                def both(q):
                    take(row_route(s, a, q))
                    take(row_route(s, 1 - a, q))
                each_piece(both)

            pl.when((t == 3) & (turn == 3) & (mod(shift, 8) == 3))(hand_on)

            @pl.when(ahead)
            def _():
                update_col(s, a_own, b_own)
                update_row(s, a_own, b_own)

        @pl.when(turn == t)
        def _():
            solve(t)

            def catch_up(p, carry):
                pl.when(jnp.logical_not(near(p)[1]))(lambda: far(p))
                return carry
            lax.fori_loop(0, t, catch_up, 0)

        stream(t)
        prompt = (mod(shift, 8) > 3) | (mod(shift, 8) < 2)
        pl.when(jnp.where(prompt, t == 2, (t == 3) & (turn != 3)))(hand_on)
        pl.when(jnp.where(prompt & ((z != 3) | (y != 0)), t == 2, t == 3))(relay_a)

        def rest(m, carry):
            p = jnp.where(t == FRONTS, jnp.where(m < 2, 2 * m, FRONTS - 1), 1)

            def one(n, carry):
                a, b = n // 2, mod(n, 2)

                @pl.when(jnp.logical_not(settled(p, a, b)))
                def _():
                    update_col(p, a, b)
                    pl.when(jnp.logical_not(put_off(p, a)))(lambda: update_row(p, a, b))
                return carry
            return lax.fori_loop(0, 4, one, carry)
        lax.fori_loop(0, jnp.where(t == FRONTS, 3, jnp.where(t == 3, 1, 0)), rest, 0)
        return carry

    lax.fori_loop(0, FRONTS + 1, front, 0)

    def last(n, carry):
        a_first, _ = near(FRONTS - 1)
        a = jnp.where(n < 2, a_first, 1 - a_first)
        b = mod(n, 2)

        def one(p, carry):
            @pl.when(put_off(p, a))
            def _():
                pl.when(b == 0)(lambda: far(p))
                pl.when(jnp.logical_not(settled(p, a, b)))(lambda: update_row(p, a, b))
            return carry
        lax.fori_loop(0, FRONTS, one, 0)
        pltpu.make_async_copy(w.at[a, b], out.at[a, :, b], out_sem.at[a, b]).start()
        return carry
    lax.fori_loop(0, 4, last, 0)

    def drain_a(a):
        for s, col in ((0, col_prev), (2, col_next), (3, col_next)):
            @pl.when(needs_a(s, r, col, a) & ((mod(shift, 8) != 3) if s == 3 else True))
            def _(s=s, col=col):
                a_copy(s, a, col, a_in.at[a]).wait_send()
    each_a(drain_a)
    leave_a(lambda copy: copy.wait_send())

    def drain_b(a, b):
        for s, row in ((0, row_next), (2, row_prev)):
            @pl.when(needs_b(s, row, c, a, b))
            def _(s=s, row=row):
                b_copy(s, a, b, row, b_in.at[0, b]).wait_send()

        @pl.when((core == 1) & needs_b(3, row_prev2, c, a, b))
        def _():
            b_copy(3, a, b, row_prev2, b_in.at[0, b]).wait_send()

        @pl.when((core == 1) & needs_b(2, r, c, a, b))
        def _():
            hand_b(a, b).wait_send()
        pltpu.make_async_copy(w.at[a, b], out.at[a, :, b], out_sem.at[a, b]).wait()
    each_ab(drain_b)

    def drain_x(s, carry):
        def one(q):
            collect(col_route(s, q)[1])
            for a in range(2):
                collect(row_route(s, a, q)[1])
        each_piece(one)
        return carry
    lax.fori_loop(0, FRONTS, drain_x, 0)


def shards(n_row, n_col, upper_a, upper_b, right_side, a_bases, b_bases, a_values, b_values):
    nb = upper_a.shape[1]
    bf16, f32 = jnp.bfloat16, jnp.float32
    b_tiles = jnp.transpose(upper_b[:3], (0, 2, 1, 3))
    c_tiles = jnp.transpose(right_side, (0, 2, 1, 3))
    dma = pltpu.SemaphoreType.DMA
    solved = pl.pallas_call(
        functools.partial(plan, nb, n_row, n_col),
        out_shape=jax.ShapeDtypeStruct((2, nb, 2, nb), f32),
        in_specs=[pl.BlockSpec(memory_space=pl.ANY)] * 7,
        out_specs=pl.BlockSpec(memory_space=pl.ANY),
        scratch_shapes=[
            pltpu.VMEM((FRONTS, 2, nb, nb), bf16),
            pltpu.VMEM((FRONTS, 2, 2, nb, nb), bf16),
            pltpu.VMEM((FRONTS, nb, nb), bf16),
            pltpu.VMEM((FRONTS, 2, nb, nb), bf16),
            pltpu.VMEM((2, 2, nb, nb), f32),
            pltpu.VMEM((2, 2, nb, nb), bf16),
            pltpu.VMEM((nb, nb), bf16),
            pltpu.VMEM((nb, nb), bf16),
            pltpu.VMEM((nb, nb), bf16),
            pltpu.VMEM((nb, nb), f32),
            pltpu.VMEM((2, nb, nb), bf16),
            pltpu.VMEM((2, nb), f32),
            pltpu.VMEM((2, nb), f32),
            dma((5,)),
            dma((2, 2)),
            dma((FRONTS, 2)),
            dma((FRONTS, 2, 2)),
            dma((FRONTS, 2)),
            dma((FRONTS, 2, 2)),
            dma((FRONTS, PIECES, 3)),
            dma((FRONTS, 2, PIECES, 5)),
            dma((FRONTS, PIECES)),
            dma((FRONTS, 2, PIECES)),
        ],
        compiler_params=pltpu.CompilerParams(
            collective_id=0, has_side_effects=True, vmem_limit_bytes=60 * 1024 * 1024
        ),
    )(upper_a, b_tiles, c_tiles, a_bases, b_bases, a_values, b_values)
    return solved


def solution(mesh):
    return jax.shard_map(
        functools.partial(shards, mesh.shape["row"], mesh.shape["col"]),
        mesh=mesh,
        in_specs=(
            P(None, "row", "col"),
            P(None, "row", None, "col"),
            P(None, "row", None, "col"),
            P(None, "row", None),
            P(None, "col", None),
            P(None, "row"),
            P(None, "col"),
        ),
        out_specs=P(None, "row", None, "col"),
        check_vma=False,
    )
```
